32 devices in a mesh: grid: 4 (over z), line: 8 (over y, x, core).
Axes of the slice: x: 2, y: 2, z: 4, core: 2. Of those that a mesh axis runs over, the one named last changes fastest.
Arguments:
- les: float32 [24, 4, 1024], P(None, 'grid', 'line'), may hold values from -6 to 6
- lines: float32 [4, 8, 128, 24, 128], P('grid', 'line'), may hold values from -6 to 6
- triplet_start: int32 [2, 4, 8, 128], P(None, 'grid', 'line'), may hold values from 0 to 80
- splice_owner: int32 [2, 4, 8, 128, 1], P(None, 'grid', 'line'), may hold values from 0 to 31; in each aligned block of 128 rows (0 to 127, 128 to 255, ..., all dimensions but the last counted through in order) at most 8 rows name the same one
- splice_line: int32 [2, 4, 8, 128], P(None, 'grid', 'line'), may hold values from 0 to 127
- splice_from: int32 [2, 4, 8, 128], P(None, 'grid', 'line'), may hold values from 0 to 7
- splice_to: int32 [2, 4, 8, 128], P(None, 'grid', 'line'), may hold values from 0 to 7
- chem_counts: int32 [4, 8, 128], P('grid', 'line'), may hold values from 1 to 6, as said below
- diffusivity: float32 [24], replicated, may hold values from 0.5 to 20
- rates: float32 [24, 24], replicated, may hold values from -1.25 to 1.25
- frozen_inverse: float32 [24, 24], replicated, may hold values from -0.3 to 0.5
Outputs:
- les_out: float32 [24, 4, 1024], P(None, 'grid', 'line')
- lines_out: float32 [4, 8, 128, 24, 128], P('grid', 'line')
The draws below stay inside these ranges and needn't reach their ends.
Inputs may be any that keep to these rules, and one draw needn't show every extreme that they name: `splice_owner`: in the rows of one device and one step no owner is named more than 8 times, a bound that some block reaches. `chem_counts`: some line has 6 substeps.
All inputs are finite; a program needn't handle non-finite values.
Results may differ from the reference program's by a relative error of at most 0.0003.
Values sent between devices are 32-bit elements; how exact they have to be, the bound alone decides.
A program may use at most 64 MiB of HBM per device.

```python
import math
import jax
import jax.numpy as jnp
import numpy as np
from jax import lax

S = 24
P_SIZE = 128
SEG = 16
TRIP = 48
KMAX = 6
STEPS = 2
CX = 1
CY = 128
LINES_DEV = 128
NX = 4
NY = 1024
NSEG = 8
CAP = 8
N_GRID = 4
N_LINE = 8
DEVICES = 32


def draw_chem_counts(key, part):
    first = jax.random.fold_in(key, 11)
    second = jax.random.fold_in(key, 12)
    ceiling = jax.random.randint(first, (N_GRID, N_LINE, 1), 1, KMAX + 1)
    ceiling = ceiling.at[0, 0, 0].set(KMAX)
    counts = 1 + jax.random.randint(second, (N_GRID, N_LINE, LINES_DEV), 0, ceiling)
    counts = counts.at[0, 0, 0].set(KMAX)
    return counts.astype(jnp.int32)


def draw_frozen_inverse(key, part):
    first = jax.random.fold_in(key, 21)
    second = jax.random.fold_in(key, 22)
    diagonal = jax.random.uniform(first, (S,), jnp.float32, 0.2, 0.5)
    off_diag = jnp.clip(0.06 * jax.random.normal(second, (S, S), jnp.float32), -0.3, 0.3)
    ident = jnp.eye(S, dtype=jnp.float32)
    return (ident * diagonal[None, :] + (1.0 - ident) * off_diag).astype(jnp.float32)


def plant(values, rng, smallest, high):
    shape = values.shape
    spot = [jax.random.randint(jax.random.fold_in(rng, axis), (), 0, shape[axis]) for axis in range(len(shape))]
    values = values.at[tuple(spot)].set(smallest)
    longest = shape.index(max(shape))
    spot[longest] = (spot[longest] + 1) % shape[longest]
    return values.at[tuple(spot)].set(high)


def block_levels(key, extent, shards, smallest, largest):
    factor_of = 1.0
    for axis_at, blocks in shards:
        heights = jax.random.uniform(jax.random.fold_in(jax.random.fold_in(key, 6), axis_at), (blocks,), jnp.float32, smallest / len(shards), largest / len(shards))
        factor_of = factor_of * jnp.repeat(jnp.exp(heights), extent[axis_at] // blocks).reshape((-1,) + (1,) * (len(extent) - 1 - axis_at))
    return factor_of


def routed_block(own_key, own, number, rows, count, top, limit, slope):
    sequence = jax.random.permutation(own_key, count)
    crowded, common = load_shares(count, rows * top, limit, slope, True), load_shares(count, rows * top, limit, slope, False)
    places = jnp.arange(count)

    def named(sizes, turn):
        used = int((sizes > 0).sum())
        fixed = max(1, used // 4)
        passed = fixed + (places - fixed + turn * (used - fixed)) % max(1, count - fixed)
        return jnp.zeros((count,), jnp.int32).at[sequence[jnp.where(places < fixed, places, passed)]].set(jnp.asarray(sizes, jnp.int32))

    sizes = jnp.where(number % 4 == 0, named(crowded, number // 4), named(common, number - number // 4 - 1))
    mixed = jax.random.permutation(jax.random.fold_in(own, 3), count)
    donor, receiver = mixed[0:count // 2 * 2:2], mixed[1:count // 2 * 2:2]
    room = jnp.minimum(sizes[donor] - 1, limit - sizes[receiver]) // 2
    room = jnp.where((donor == sequence[0]) | (receiver == sequence[0]) | (sizes[receiver] == 0), 0, jnp.maximum(room, 0))
    passed = jax.random.randint(jax.random.fold_in(own, 4), (count // 2,), 0, 1 << 20) % (room + 1)
    sizes = sizes.at[donor].add(-passed).at[receiver].add(passed)
    labels = jnp.searchsorted(jnp.cumsum(sizes), jnp.arange(rows * top), side="right").astype(jnp.int32)
    listing = labels.reshape(top, rows).T
    listing = listing[jax.random.permutation(jax.random.fold_in(own, 1), rows)]
    turn = jax.random.randint(jax.random.fold_in(own, 2), (rows, 1), 0, top)
    return jnp.take_along_axis(listing, (jnp.arange(top)[None, :] + turn) % top, axis=1)


def load_shares(number_of, total, most, slope, full):
    loads = [(1 << 20) // math.isqrt(grade ** slope) + 1 for grade in range(1, number_of + 1)]
    largest = most if full else min(most, max(-(-total // number_of), total * loads[0] // sum(loads)))
    least = 1 if total - largest >= number_of - 1 else 0
    given, spare = [largest] + [least] * (number_of - 1), total - largest - least * (number_of - 1)
    while spare > 0:
        free = [i for i in range(1, number_of) if given[i] < largest] or [i for i in range(1, number_of) if given[i] < most]
        pool, left = sum([loads[i] for i in free]), spare
        for i in free:
            addition = min(most - given[i], max(1, left * loads[i] // pool), spare)
            given[i] = given[i] + addition
            spare = spare - addition
    return np.array(given)


def centred(rng, dims, width, bound, shards=(), held_as=jnp.bfloat16):
    drawn = width * jax.random.normal(rng, dims, jnp.float32)
    if shards:
        drawn = drawn * block_levels(rng, dims, shards, -0.22, 0.18)
    return jnp.clip(drawn, -bound, bound).astype(held_as)


def setup_inputs(seed: int = 0) -> dict:
    key_of = jax.random.split(jax.random.key(seed), 12)
    les = centred(key_of[0], (S, NX, NY), 1.0, 6.0, ((1, 4), (2, 8)), jnp.float32)
    lines = centred(key_of[1], (N_GRID, N_LINE, LINES_DEV, S, P_SIZE), 1.0, 6.0, ((0, 4), (1, 8)), jnp.float32)
    triplet_start = plant(jax.random.randint(key_of[2], (STEPS, N_GRID, N_LINE, LINES_DEV), 0, P_SIZE - TRIP + 1), jax.random.fold_in(key_of[2], 1), 0, P_SIZE - TRIP).astype(jnp.int32)
    splice_owner_keys = jax.random.split(jax.random.fold_in(key_of[3], 1), STEPS * N_GRID * N_LINE * LINES_DEV // LINES_DEV)
    splice_owner_turns = jax.random.permutation(jax.random.fold_in(key_of[3], 3), STEPS * N_GRID * N_LINE * LINES_DEV // LINES_DEV)
    splice_owner = jax.vmap(lambda own, number: routed_block(jax.random.fold_in(key_of[3], 2), own, number, LINES_DEV, DEVICES, 1, CAP, 2))(splice_owner_keys, splice_owner_turns).reshape((STEPS, N_GRID, N_LINE, LINES_DEV, 1))
    splice_line = plant(jax.random.randint(key_of[4], (STEPS, N_GRID, N_LINE, LINES_DEV), 0, LINES_DEV), jax.random.fold_in(key_of[4], 1), 0, LINES_DEV - 1).astype(jnp.int32)
    splice_from = plant(jax.random.randint(key_of[5], (STEPS, N_GRID, N_LINE, LINES_DEV), 0, NSEG), jax.random.fold_in(key_of[5], 1), 0, NSEG - 1).astype(jnp.int32)
    splice_to = plant(jax.random.randint(key_of[6], (STEPS, N_GRID, N_LINE, LINES_DEV), 0, NSEG), jax.random.fold_in(key_of[6], 1), 0, NSEG - 1).astype(jnp.int32)
    chem_counts = draw_chem_counts(jax.random.fold_in(key_of[11], 71), 0)
    diffusivity = jnp.clip(jnp.exp(jax.random.uniform(key_of[8], (S,), jnp.float32, math.log(0.5), math.log(20.0))), 0.5, 20.0)
    rates = centred(key_of[9], (S, S), S ** -0.5, 1.25, (), jnp.float32)
    frozen_inverse = draw_frozen_inverse(jax.random.fold_in(key_of[11], 71), 0)
    return dict(les=les, lines=lines, triplet_start=triplet_start, splice_owner=splice_owner, splice_line=splice_line, splice_from=splice_from, splice_to=splice_to, chem_counts=chem_counts, diffusivity=diffusivity, rates=rates, frozen_inverse=frozen_inverse)


les_rate = 0.2
relax_rate = 0.5
splice_weight = 0.5

def diffusion_inverse(diffusivity, points):
    place = jnp.arange(points)
    ends = ((place == 0) | (place == points - 1)).astype(jnp.float32)
    coeff = diffusivity[:, None]
    main = 1.0 + coeff * (2.0 - ends[None, :])
    off_diag = -coeff * jnp.ones((1, points), jnp.float32)
    lower = jnp.where(place[None, :] == 0, jnp.float32(0.0), off_diag)
    upper = jnp.where(place[None, :] == points - 1, jnp.float32(0.0), off_diag)
    ident = jnp.broadcast_to(jnp.eye(points, dtype=jnp.float32), (diffusivity.shape[0], points, points))
    return lax.linalg.tridiagonal_solve(lower, main, upper, ident)

def triplet_index(start, points, length):
    place = jnp.arange(points).astype(jnp.int32)
    rel = place[None, :] - start[:, None].astype(jnp.int32)
    third = length // 3
    source = jnp.where(rel < third, 3 * rel, jnp.where(rel < 2 * third, 3 * (2 * third - 1 - rel) + 1, 3 * (rel - 2 * third) + 2))
    inside = (rel >= 0) & (rel < length)
    return jnp.where(inside, source + start[:, None].astype(jnp.int32), place[None, :]).astype(jnp.int32)

def chemistry(state, counts, rates, frozen_inverse):
    for sub in range(KMAX):
        active = (counts > sub)[:, None, None]
        source = jnp.einsum('st,ltp->lsp', rates, jnp.tanh(state), precision=lax.Precision.HIGHEST)
        change = jnp.einsum('st,ltp->lsp', frozen_inverse, source, precision=lax.Precision.HIGHEST)
        state = jnp.where(active, state + change, state)
    return state

def reference(les, lines, triplet_start, splice_owner, splice_line, splice_from, splice_to, chem_counts, diffusivity, rates, frozen_inverse):
    inverse = diffusion_inverse(diffusivity, P_SIZE)
    total = N_GRID * N_LINE * LINES_DEV
    field = les
    state = lines.reshape(total, S, P_SIZE)
    counts = chem_counts.reshape(total)
    rows = jnp.arange(total).astype(jnp.int32)
    for step in range(STEPS):
        padded = jnp.pad(field, ((0, 0), (1, 1), (1, 1)))
        beside = padded[:, 2:, 1:-1] + padded[:, :-2, 1:-1] + padded[:, 1:-1, 2:] + padded[:, 1:-1, :-2]
        mid = field + les_rate * (beside - 4.0 * field)
        cellwise = mid.reshape(S, N_GRID, CX, N_LINE, CY).transpose(1, 3, 2, 4, 0).reshape(total, S)
        state = state + relax_rate * (cellwise - jnp.mean(state, axis=2))[:, :, None]
        index = triplet_index(triplet_start[step].reshape(total), P_SIZE, TRIP)
        state = jnp.take_along_axis(state, index[:, None, :], axis=2)
        state = jnp.einsum('lsp,sqp->lsq', state, inverse, precision=lax.Precision.HIGHEST)
        state = chemistry(state, counts, rates, frozen_inverse)
        four = state.reshape(total, S, NSEG, SEG)
        outgoing = four[rows, :, splice_from[step].reshape(total).astype(jnp.int32), :]
        target = (splice_owner[step].reshape(total) * LINES_DEV + splice_line[step].reshape(total)).astype(jnp.int32)
        landing = splice_to[step].reshape(total).astype(jnp.int32)
        previous = four[target, :, landing, :]
        four = four.at[target, :, landing, :].add(splice_weight * (outgoing - previous))
        state = four.reshape(total, S, P_SIZE)
        filtered = jnp.mean(state, axis=2)
        back = filtered.reshape(N_GRID, N_LINE, CX, CY, S).transpose(4, 0, 2, 1, 3).reshape(S, NX, NY)
        field = 0.5 * mid + 0.5 * back
    return (field, state.reshape(lines.shape))
```

```python
import functools

import jax
import jax.numpy as jnp
from jax import lax
from jax.experimental import pallas as pl
from jax.experimental.pallas import tpu as pltpu
from jax.sharding import PartitionSpec as P

SEG = 16
TRIP = 48
STEPS = 2

les_rate = 0.2
relax_rate = 0.5
splice_weight = 0.5

VMEM = pl.BlockSpec(memory_space=pltpu.VMEM)
SMEM = pl.BlockSpec(memory_space=pltpu.SMEM)


def shift_along(array, axis, dim):
    peers, length = lax.axis_size(axis), array.shape[dim]
    up = [(i, i + 1) for i in range(peers - 1)]
    down = [(j, i) for i, j in up]
    before = lax.ppermute(lax.slice_in_dim(array, length - 1, length, axis=dim), axis, up)
    after = lax.ppermute(lax.slice_in_dim(array, 0, 1, axis=dim), axis, down)
    lower = jnp.concatenate([before, lax.slice_in_dim(array, 0, length - 1, axis=dim)], axis=dim)
    upper = jnp.concatenate([lax.slice_in_dim(array, 1, length, axis=dim), after], axis=dim)
    return lower + upper


def diffusion_inverse(diffusivity, points):
    coeff = diffusivity[:, None]
    root = jnp.sqrt(4.0 * coeff + 1.0)
    theta = -jnp.log(2.0 * coeff / (2.0 * coeff + 1.0 + root))
    place = jnp.arange(points, dtype=jnp.float32)
    low = 1.0 + jnp.exp(-(2.0 * place + 1.0)[None, :] * theta)
    high = 1.0 + jnp.exp(-(2.0 * (points - place) - 1.0)[None, :] * theta)
    scale = 1.0 / (root * (1.0 - jnp.exp(-2.0 * points * theta)))
    apart = jnp.abs(place[:, None] - place[None, :])
    ends = jnp.where(
        (place[:, None] <= place[None, :])[None],
        low[:, :, None] * high[:, None, :],
        low[:, None, :] * high[:, :, None],
    )
    return jnp.exp(-apart[None] * theta[:, :, None]) * ends * scale[:, :, None]


def halves(value):
    top = value.astype(jnp.bfloat16)
    return top, (value - top.astype(jnp.float32)).astype(jnp.bfloat16)


def diffuse_kernel(species, x_ref, start_ref, m_ref, o_ref):
    points = x_ref.shape[1]
    lines = x_ref.shape[0] // species
    start = start_ref[...]
    place = lax.broadcasted_iota(jnp.int32, (lines, points), 1)
    rel = place - start
    third = TRIP // 3
    source = jnp.where(
        rel < third,
        3 * rel,
        jnp.where(rel < 2 * third, 3 * (2 * third - 1 - rel) + 1, 3 * (rel - 2 * third) + 2),
    )
    index = jnp.where((rel >= 0) & (rel < TRIP), source + start, place)

    def one(s, carry):
        y = x_ref[pl.ds(s, lines, stride=species), :]
        y = jnp.take_along_axis(y, index, axis=1, mode="promise_in_bounds")
        top, rest = halves(y)
        mtop, mrest = halves(m_ref[s])
        dot = functools.partial(jnp.dot, preferred_element_type=jnp.float32)
        out = dot(top, mtop) + dot(rest, mtop) + dot(top, mrest)
        o_ref[pl.ds(s, lines, stride=species), :] = out
        return carry

    lax.fori_loop(0, species, one, 0, unroll=4)


def chem_kernel(chunk, y_ref, mid_ref, a_ref, turns_ref, counts_ref, owner_ref, rank_ref, from_ref, o_ref, send_ref):
    lines, species, points = y_ref.shape
    lane = lax.broadcasted_iota(jnp.int32, (species, points), 1)
    send_ref[...] = jnp.zeros_like(send_ref)
    mid = mid_ref[...]

    def lift(l, carry):
        add = jnp.take_along_axis(mid, jnp.full((species, points), l, jnp.int32), axis=1, mode="promise_in_bounds")
        o_ref[l] = y_ref[l] + relax_rate * add
        return carry

    lax.fori_loop(0, lines, lift, 0, unroll=8)
    matrix = a_ref[...]

    def substep(sub, carry):
        def part(c, inner):
            base = c * chunk
            for q in range(0, chunk, 4):
                columns = []
                state = []
                for h in (0, 2):
                    y = o_ref[pl.ds(base + q + h, 2)].reshape(2 * species, points)
                    state.append(y)
                    top, rest = halves(jnp.tanh(y))
                    columns.append(jnp.concatenate([top, top, rest], axis=0))
                right = jnp.concatenate(columns, axis=1)
                change = jnp.dot(matrix, right, preferred_element_type=jnp.float32)
                for h in (0, 1):
                    for k in (0, 1):
                        l = base + q + 2 * h + k
                        factor = jnp.where(counts_ref[l] > sub, jnp.float32(1.0), jnp.float32(0.0))
                        rows = slice(k * species, (k + 1) * species)
                        o_ref[l] = state[h][rows] + factor * change[rows, h * points : (h + 1) * points]
            return inner

        return lax.fori_loop(0, lines // chunk, part, carry)

    lax.fori_loop(0, turns_ref[0], substep, 0)

    def pack(l, carry):
        slot = rank_ref[l]
        owner = owner_ref[l]
        move = (SEG * (slot - from_ref[l])) & (points - 1)
        value = pltpu.roll(o_ref[l], move, 1)
        send_ref[owner] = jnp.where(lane // SEG == slot, value, send_ref[owner])
        return carry

    lax.fori_loop(0, lines, pack, 0, unroll=8)


def land_kernel(slots, y_ref, recv_ref, aim_ref, mid_ref, o_ref, les_ref):
    lines, species, points = y_ref.shape
    groups = recv_ref.shape[0]
    segments = points // SEG
    lane = lax.broadcasted_iota(jnp.int32, (species, points), 1)
    o_ref[...] = y_ref[...]

    def land(r, carry):
        got = recv_ref[r]
        for k in range(slots):
            code = aim_ref[r * slots + k]
            safe = jnp.maximum(code, 0)
            line = safe // segments
            seg = safe - line * segments
            value = pltpu.roll(got, (SEG * (seg - k)) & (points - 1), 1)
            hit = lane // SEG == jnp.where(code >= 0, seg, -1)
            o_ref[line] = o_ref[line] + jnp.where(hit, splice_weight * (value - y_ref[line]), 0.0)
        return carry

    lax.fori_loop(0, groups, land, 0)

    def filtered(l, total):
        return jnp.where(lane == l, jnp.sum(o_ref[l], axis=1, keepdims=True), total)

    total = lax.fori_loop(0, lines, filtered, jnp.zeros((species, points), jnp.float32), unroll=8)
    les_ref[...] = 0.5 * mid_ref[...] + (0.5 / points) * total


def body(
    les,
    lines,
    triplet_start,
    splice_owner,
    splice_line,
    splice_from,
    splice_to,
    chem_counts,
    diffusivity,
    rates,
    frozen_inverse,
):
    groups = lax.axis_size("grid") * lax.axis_size("line")
    _, _, count, species, points = lines.shape
    segments = points // SEG
    slots = min(segments, max(2, 2 * count // groups))
    f32 = jnp.float32
    params = pltpu.CompilerParams(vmem_limit_bytes=40 * 1024 * 1024)

    mixing = diffusion_inverse(diffusivity, points) - relax_rate / points
    joint = jnp.dot(frozen_inverse, rates, precision=lax.Precision.HIGHEST)
    twice = jnp.kron(jnp.eye(2, dtype=f32), joint)
    top = lax.reduce_precision(twice, 8, 7)
    rest = lax.reduce_precision(twice - top, 8, 7)
    matrix = jnp.concatenate([top, rest, top], axis=1).astype(jnp.bfloat16)

    starts = triplet_start.reshape(STEPS, count, 1)
    owner = splice_owner.reshape(STEPS, count)
    line_to = splice_line.reshape(STEPS, count)
    seg_from = splice_from.reshape(STEPS, count)
    seg_to = splice_to.reshape(STEPS, count)
    counts = chem_counts.reshape(count)
    turns = jnp.max(counts).reshape(1)
    order = jnp.arange(count)
    earlier = (owner[:, :, None] == owner[:, None, :]) & (order[None, :, None] > order[None, None, :])
    rank = jnp.sum(earlier.astype(jnp.int32), axis=2)
    position = owner * slots + rank
    code = (line_to * segments + seg_to).astype(f32)
    hit = jnp.arange(groups * slots)[None, :, None] == position[:, None, :]
    aims = jnp.max(jnp.where(hit, code[:, None, :], -1.0), axis=2)
    aims = aims.reshape(STEPS, groups, slots).transpose(1, 0, 2)
    aims = lax.all_to_all(aims, ("grid", "line"), split_axis=0, concat_axis=0, tiled=True)
    aims = aims.transpose(1, 0, 2).reshape(STEPS, groups * slots).astype(jnp.int32)

    diffuse = pl.pallas_call(
        functools.partial(diffuse_kernel, species),
        out_shape=jax.ShapeDtypeStruct((count * species, points), f32),
        in_specs=[VMEM] * 3,
        out_specs=VMEM,
        compiler_params=params,
        cost_estimate=pl.CostEstimate(flops=6 * species * count * points * points, bytes_accessed=5 << 20, transcendentals=0),
        name="diffuse",
    )
    block = jax.ShapeDtypeStruct((count, species, points), f32)
    chem = pl.pallas_call(
        functools.partial(chem_kernel, 32),
        out_shape=(block, jax.ShapeDtypeStruct((groups, species, points), f32)),
        in_specs=[VMEM] * 3 + [SMEM] * 5,
        out_specs=(VMEM, VMEM),
        compiler_params=params,
        name="chem",
    )
    land = pl.pallas_call(
        functools.partial(land_kernel, slots),
        out_shape=(block, jax.ShapeDtypeStruct((species, count), f32)),
        in_specs=[VMEM, VMEM, SMEM, VMEM],
        out_specs=(VMEM, VMEM),
        compiler_params=params,
        name="land",
    )

    field = les
    state = lines.reshape(count, species, points)
    for step in range(STEPS):
        beside = shift_along(field, "grid", 1) + shift_along(field, "line", 2)
        mid = (field + les_rate * (beside - 4.0 * field)).reshape(species, count)
        spread = diffuse(state.reshape(count * species, points), starts[step], mixing)
        state, sending = chem(
            spread.reshape(count, species, points), mid, matrix, turns, counts, owner[step], rank[step], seg_from[step]
        )
        received = lax.all_to_all(sending, ("grid", "line"), split_axis=0, concat_axis=0, tiled=True)
        state, field = land(state, received, aims[step], mid)
        field = field.reshape(les.shape)
    return (field, state.reshape(lines.shape))


def solution(mesh):
    in_specs = (
        P(None, "grid", "line"),
        P("grid", "line", None, None, None),
        P(None, "grid", "line", None),
        P(None, "grid", "line", None, None),
        P(None, "grid", "line", None),
        P(None, "grid", "line", None),
        P(None, "grid", "line", None),
        P("grid", "line", None),
        P(),
        P(),
        P(),
    )
    out_specs = (P(None, "grid", "line"), P("grid", "line", None, None, None))
    return jax.shard_map(body, mesh=mesh, in_specs=in_specs, out_specs=out_specs, check_vma=False)
```

```python
import functools

import jax
import jax.numpy as jnp
from jax import lax
from jax.experimental import pallas as pl
from jax.experimental.pallas import tpu as pltpu
from jax.sharding import PartitionSpec as P

SEG = 16
TRIP = 48
STEPS = 2

les_rate = 0.2
relax_rate = 0.5
splice_weight = 0.5

VMEM = pl.BlockSpec(memory_space=pltpu.VMEM)
SMEM = pl.BlockSpec(memory_space=pltpu.SMEM)


def shift_along(array, axis, dim):
    peers, length = lax.axis_size(axis), array.shape[dim]
    up = [(i, i + 1) for i in range(peers - 1)]
    down = [(j, i) for i, j in up]
    before = lax.ppermute(lax.slice_in_dim(array, length - 1, length, axis=dim), axis, up)
    after = lax.ppermute(lax.slice_in_dim(array, 0, 1, axis=dim), axis, down)
    lower = jnp.concatenate([before, lax.slice_in_dim(array, 0, length - 1, axis=dim)], axis=dim)
    upper = jnp.concatenate([lax.slice_in_dim(array, 1, length, axis=dim), after], axis=dim)
    return lower + upper


def diffusion_inverse(diffusivity, points):
    coeff = diffusivity[:, None]
    root = jnp.sqrt(4.0 * coeff + 1.0)
    theta = -jnp.log(2.0 * coeff / (2.0 * coeff + 1.0 + root))
    place = jnp.arange(points, dtype=jnp.float32)
    low = 1.0 + jnp.exp(-(2.0 * place + 1.0)[None, :] * theta)
    high = 1.0 + jnp.exp(-(2.0 * (points - place) - 1.0)[None, :] * theta)
    scale = 1.0 / (root * (1.0 - jnp.exp(-2.0 * points * theta)))
    apart = jnp.abs(place[:, None] - place[None, :])
    ends = jnp.where(
        (place[:, None] <= place[None, :])[None],
        low[:, :, None] * high[:, None, :],
        low[:, None, :] * high[:, :, None],
    )
    return jnp.exp(-apart[None] * theta[:, :, None]) * ends * scale[:, :, None]


def halves(value):
    top = value.astype(jnp.bfloat16)
    return top, (value - top.astype(jnp.float32)).astype(jnp.bfloat16)


def diffuse_kernel(species, x_ref, start_ref, m_ref, o_ref):
    points = x_ref.shape[1]
    lines = x_ref.shape[0] // species
    start = start_ref[...]
    place = lax.broadcasted_iota(jnp.int32, (lines, points), 1)
    rel = place - start
    third = TRIP // 3
    source = jnp.where(
        rel < third,
        3 * rel,
        jnp.where(rel < 2 * third, 3 * (2 * third - 1 - rel) + 1, 3 * (rel - 2 * third) + 2),
    )
    index = jnp.where((rel >= 0) & (rel < TRIP), source + start, place)

    def one(s, carry):
        y = x_ref[pl.ds(s, lines, stride=species), :]
        y = jnp.take_along_axis(y, index, axis=1, mode="promise_in_bounds")
        top, rest = halves(y)
        mtop, mrest = halves(m_ref[s])
        dot = functools.partial(jnp.dot, preferred_element_type=jnp.float32)
        out = dot(top, mtop) + dot(rest, mtop) + dot(top, mrest)
        o_ref[pl.ds(s, lines, stride=species), :] = out
        return carry

    lax.fori_loop(0, species, one, 0, unroll=4)


def chem_kernel(chunk, y_ref, mid_ref, a_ref, turns_ref, counts_ref, owner_ref, rank_ref, from_ref, o_ref, send_ref, other_ref):
    lines, species, points = y_ref.shape
    lane = lax.broadcasted_iota(jnp.int32, (species, points), 1)
    send_ref[...] = jnp.zeros_like(send_ref)
    mid = mid_ref[...]

    def lift(l, carry):
        add = jnp.take_along_axis(mid, jnp.full((species, points), l, jnp.int32), axis=1, mode="promise_in_bounds")
        o_ref[l] = y_ref[l] + relax_rate * add
        return carry

    lax.fori_loop(0, lines, lift, 0, unroll=8)
    matrix = a_ref[...]

    def substep(sub, in_ref, out_ref):
        def part(c, inner):
            base = c * chunk
            for q in range(0, chunk, 4):
                columns = []
                state = []
                for h in (0, 2):
                    y = in_ref[pl.ds(base + q + h, 2)].reshape(2 * species, points)
                    state.append(y)
                    top, rest = halves(jnp.tanh(y))
                    columns.append(jnp.concatenate([top, top, rest], axis=0))
                right = jnp.concatenate(columns, axis=1)
                change = jnp.dot(matrix, right, preferred_element_type=jnp.float32)
                for h in (0, 1):
                    for k in (0, 1):
                        l = base + q + 2 * h + k
                        factor = jnp.where(counts_ref[l] > sub, jnp.float32(1.0), jnp.float32(0.0))
                        rows = slice(k * species, (k + 1) * species)
                        out_ref[l] = state[h][rows] + factor * change[rows, h * points : (h + 1) * points]
            return inner

        lax.fori_loop(0, lines // chunk, part, 0)

    def two(pair, carry):
        substep(2 * pair, o_ref, other_ref)
        substep(2 * pair + 1, other_ref, o_ref)
        return carry

    lax.fori_loop(0, (turns_ref[0] + 1) // 2, two, 0)

    def pack(l, carry):
        slot = rank_ref[l]
        owner = owner_ref[l]
        move = (SEG * (slot - from_ref[l])) & (points - 1)
        value = pltpu.roll(o_ref[l], move, 1)
        send_ref[owner] = jnp.where(lane // SEG == slot, value, send_ref[owner])
        return carry

    lax.fori_loop(0, lines, pack, 0, unroll=8)


def swap_kernel(names, groups, pairs, *refs):
    sends, takes = refs[:pairs], refs[pairs : 2 * pairs]
    send_sem, recv_sem, own_sem = refs[2 * pairs :]
    width = lax.axis_size(names[1])
    me = lax.axis_index(names[0]) * width + lax.axis_index(names[1])

    def place(j):
        peer = lax.rem(me + j, groups)
        return peer, (peer // width, lax.rem(peer, width))

    barrier = pltpu.get_barrier_semaphore()

    def greet(j, carry):
        pl.semaphore_signal(barrier, inc=1, device_id=place(j)[1], device_id_type=pl.DeviceIdType.MESH)
        return carry

    lax.fori_loop(1, groups, greet, 0)
    own = [pltpu.make_async_copy(sends[p].at[me], takes[p].at[me], own_sem.at[p]) for p in range(pairs)]
    for copy in own:
        copy.start()
    pl.semaphore_wait(barrier, groups - 1)

    def copies(j):
        peer, device = place(j)
        return [
            pltpu.make_async_remote_copy(
                src_ref=sends[p].at[peer],
                dst_ref=takes[p].at[me],
                send_sem=send_sem.at[p, j],
                recv_sem=recv_sem.at[p, j],
                device_id=device,
                device_id_type=pl.DeviceIdType.MESH,
            )
            for p in range(pairs)
        ]

    def begin(j, carry):
        for copy in copies(j):
            copy.start()
        return carry

    def finish(j, carry):
        for copy in copies(j):
            copy.wait()
        return carry

    lax.fori_loop(1, groups, begin, 0)
    for copy in own:
        copy.wait()
    lax.fori_loop(1, groups, finish, 0)


def swap(arrays, number):
    names = ("grid", "line")
    groups = arrays[0].shape[0]
    pairs = len(arrays)
    return pl.pallas_call(
        functools.partial(swap_kernel, names, groups, pairs),
        out_shape=[jax.ShapeDtypeStruct(a.shape, a.dtype) for a in arrays],
        in_specs=[VMEM] * pairs,
        out_specs=[VMEM] * pairs,
        scratch_shapes=[
            pltpu.SemaphoreType.DMA((pairs, groups)),
            pltpu.SemaphoreType.DMA((pairs, groups)),
            pltpu.SemaphoreType.DMA((pairs,)),
        ],
        compiler_params=pltpu.CompilerParams(collective_id=number, has_side_effects=True),
        name="swap%d" % number,
    )(*arrays)


def land_kernel(step, slots, y_ref, recv_ref, aim_ref, mid_ref, o_ref, les_ref):
    lines, species, points = y_ref.shape
    groups = recv_ref.shape[0]
    segments = points // SEG
    lane = lax.broadcasted_iota(jnp.int32, (species, points), 1)
    o_ref[...] = y_ref[...]

    def land(r, carry):
        got = recv_ref[r]
        for k in range(slots):
            code = aim_ref[r, 0, step * slots + k]
            safe = jnp.maximum(code, 0)
            line = safe // segments
            seg = safe - line * segments
            value = pltpu.roll(got, (SEG * (seg - k)) & (points - 1), 1)
            hit = lane // SEG == jnp.where(code >= 0, seg, -1)
            o_ref[line] = o_ref[line] + jnp.where(hit, splice_weight * (value - y_ref[line]), 0.0)
        return carry

    lax.fori_loop(0, groups, land, 0)

    def filtered(l, total):
        return jnp.where(lane == l, jnp.sum(o_ref[l], axis=1, keepdims=True), total)

    total = lax.fori_loop(0, lines, filtered, jnp.zeros((species, points), jnp.float32), unroll=8)
    les_ref[...] = 0.5 * mid_ref[...] + (0.5 / points) * total


def body(
    les,
    lines,
    triplet_start,
    splice_owner,
    splice_line,
    splice_from,
    splice_to,
    chem_counts,
    diffusivity,
    rates,
    frozen_inverse,
):
    groups = lax.axis_size("grid") * lax.axis_size("line")
    _, _, count, species, points = lines.shape
    segments = points // SEG
    slots = min(segments, max(2, 2 * count // groups))
    f32 = jnp.float32
    params = pltpu.CompilerParams(vmem_limit_bytes=40 * 1024 * 1024)

    mixing = diffusion_inverse(diffusivity, points) - relax_rate / points
    joint = jnp.dot(frozen_inverse, rates, precision=lax.Precision.HIGHEST)
    twice = jnp.kron(jnp.eye(2, dtype=f32), joint)
    top = lax.reduce_precision(twice, 8, 7)
    rest = lax.reduce_precision(twice - top, 8, 7)
    matrix = jnp.concatenate([top, rest, top], axis=1).astype(jnp.bfloat16)

    starts = triplet_start.reshape(STEPS, count, 1)
    owner = splice_owner.reshape(STEPS, count)
    line_to = splice_line.reshape(STEPS, count)
    seg_from = splice_from.reshape(STEPS, count)
    seg_to = splice_to.reshape(STEPS, count)
    counts = chem_counts.reshape(count)
    turns = jnp.max(counts).reshape(1)
    order = jnp.arange(count)
    earlier = (owner[:, :, None] == owner[:, None, :]) & (order[None, :, None] > order[None, None, :])
    rank = jnp.sum(earlier.astype(jnp.int32), axis=2)
    position = owner * slots + rank
    code = line_to * segments + seg_to
    hit = jnp.arange(groups * slots)[None, :, None] == position[:, None, :]
    aims = jnp.max(jnp.where(hit, code[:, None, :], -1), axis=2)
    aims = aims.reshape(STEPS, groups, slots).transpose(1, 0, 2).reshape(groups, 1, STEPS * slots)
    aims = jnp.pad(aims, ((0, 0), (0, 0), (0, points - STEPS * slots)))

    diffuse = pl.pallas_call(
        functools.partial(diffuse_kernel, species),
        out_shape=jax.ShapeDtypeStruct((count * species, points), f32),
        in_specs=[VMEM] * 3,
        out_specs=VMEM,
        compiler_params=params,
        cost_estimate=pl.CostEstimate(flops=6 * species * count * points * points, bytes_accessed=5 << 20, transcendentals=0),
        name="diffuse",
    )
    block = jax.ShapeDtypeStruct((count, species, points), f32)
    chem = pl.pallas_call(
        functools.partial(chem_kernel, 32),
        out_shape=(block, jax.ShapeDtypeStruct((groups, species, points), f32)),
        in_specs=[VMEM] * 3 + [SMEM] * 5,
        out_specs=(VMEM, VMEM),
        scratch_shapes=[pltpu.VMEM((count, species, points), f32)],
        compiler_params=params,
        name="chem",
    )
    def land(step, *given):
        return pl.pallas_call(
            functools.partial(land_kernel, step, slots),
            out_shape=(block, jax.ShapeDtypeStruct((species, count), f32)),
            in_specs=[VMEM, VMEM, SMEM, VMEM],
            out_specs=(VMEM, VMEM),
            compiler_params=params,
            name="land",
        )(*given)

    field = les
    state = lines.reshape(count, species, points)
    for step in range(STEPS):
        beside = shift_along(field, "grid", 1) + shift_along(field, "line", 2)
        mid = (field + les_rate * (beside - 4.0 * field)).reshape(species, count)
        spread = diffuse(state.reshape(count * species, points), starts[step], mixing)
        state, sending = chem(
            spread.reshape(count, species, points), mid, matrix, turns, counts, owner[step], rank[step], seg_from[step]
        )
        if step == 0:
            received, aims = swap([sending, aims], 0)
        else:
            (received,) = swap([sending], step)
        state, field = land(step, state, received, aims, mid)
        field = field.reshape(les.shape)
    return (field, state.reshape(lines.shape))


def solution(mesh):
    in_specs = (
        P(None, "grid", "line"),
        P("grid", "line", None, None, None),
        P(None, "grid", "line", None),
        P(None, "grid", "line", None, None),
        P(None, "grid", "line", None),
        P(None, "grid", "line", None),
        P(None, "grid", "line", None),
        P("grid", "line", None),
        P(),
        P(),
        P(),
    )
    out_specs = (P(None, "grid", "line"), P("grid", "line", None, None, None))
    return jax.shard_map(body, mesh=mesh, in_specs=in_specs, out_specs=out_specs, check_vma=False)
```

```python
import functools

import jax
import jax.numpy as jnp
from jax import lax
from jax.experimental import pallas as pl
from jax.experimental.pallas import tpu as pltpu
from jax.sharding import PartitionSpec as P

SEG = 16
TRIP = 48
STEPS = 2

les_rate = 0.2
relax_rate = 0.5
splice_weight = 0.5

VMEM = pl.BlockSpec(memory_space=pltpu.VMEM)
SMEM = pl.BlockSpec(memory_space=pltpu.SMEM)


def rim_kernel(names, x_ref, o_ref, send_sem, recv_sem):
    at = [lax.axis_index(n) for n in names]
    size = [lax.axis_size(n) for n in names]
    devices = []
    for axis in (0, 1):
        for move in (1, size[axis] - 1):
            there = list(at)
            there[axis] = lax.rem(at[axis] + move, size[axis])
            devices.append(tuple(there))
    barrier = pltpu.get_barrier_semaphore()
    for device in devices:
        pl.semaphore_signal(barrier, inc=1, device_id=device, device_id_type=pl.DeviceIdType.MESH)
    pl.semaphore_wait(barrier, 4)
    copies = [
        pltpu.make_async_remote_copy(
            src_ref=x_ref,
            dst_ref=o_ref.at[k],
            send_sem=send_sem.at[k],
            recv_sem=recv_sem.at[k],
            device_id=devices[k],
            device_id_type=pl.DeviceIdType.MESH,
        )
        for k in range(4)
    ]
    for copy in copies:
        copy.start()
    for copy in copies:
        copy.wait()


def neighbours(field, number):
    species, cx, cy = field.shape
    flat = field.reshape(species, cx * cy)
    names = ("grid", "line")
    got = pl.pallas_call(
        functools.partial(rim_kernel, names),
        out_shape=jax.ShapeDtypeStruct((4,) + flat.shape, flat.dtype),
        in_specs=[VMEM],
        out_specs=VMEM,
        scratch_shapes=[pltpu.SemaphoreType.DMA((4,)), pltpu.SemaphoreType.DMA((4,))],
        compiler_params=pltpu.CompilerParams(collective_id=number, has_side_effects=True),
        name="rim%d" % number,
    )(flat).reshape((4,) + field.shape)
    total = 0.0
    for axis, dim in (("grid", 1), ("line", 2)):
        peers, length, at = lax.axis_size(axis), field.shape[dim], lax.axis_index(axis)
        before = lax.slice_in_dim(got[2 * dim - 2], length - 1, length, axis=dim)
        after = lax.slice_in_dim(got[2 * dim - 1], 0, 1, axis=dim)
        before = jnp.where(at > 0, before, 0.0)
        after = jnp.where(at < peers - 1, after, 0.0)
        total += jnp.concatenate([before, lax.slice_in_dim(field, 0, length - 1, axis=dim)], axis=dim)
        total += jnp.concatenate([lax.slice_in_dim(field, 1, length, axis=dim), after], axis=dim)
    return total


def diffusion_inverse(diffusivity, points):
    coeff = diffusivity[:, None]
    root = jnp.sqrt(4.0 * coeff + 1.0)
    theta = -jnp.log(2.0 * coeff / (2.0 * coeff + 1.0 + root))
    place = jnp.arange(points, dtype=jnp.float32)
    low = 1.0 + jnp.exp(-(2.0 * place + 1.0)[None, :] * theta)
    high = 1.0 + jnp.exp(-(2.0 * (points - place) - 1.0)[None, :] * theta)
    scale = 1.0 / (root * (1.0 - jnp.exp(-2.0 * points * theta)))
    apart = jnp.abs(place[:, None] - place[None, :])
    ends = jnp.where(
        (place[:, None] <= place[None, :])[None],
        low[:, :, None] * high[:, None, :],
        low[:, None, :] * high[:, :, None],
    )
    return jnp.exp(-apart[None] * theta[:, :, None]) * ends * scale[:, :, None]


def halves(value):
    top = value.astype(jnp.bfloat16)
    return top, (value - top.astype(jnp.float32)).astype(jnp.bfloat16)


def diffuse_kernel(species, x_ref, start_ref, m_ref, o_ref):
    points = x_ref.shape[1]
    lines = x_ref.shape[0] // species
    start = start_ref[...]
    place = lax.broadcasted_iota(jnp.int32, (lines, points), 1)
    rel = place - start
    third = TRIP // 3
    source = jnp.where(
        rel < third,
        3 * rel,
        jnp.where(rel < 2 * third, 3 * (2 * third - 1 - rel) + 1, 3 * (rel - 2 * third) + 2),
    )
    index = jnp.where((rel >= 0) & (rel < TRIP), source + start, place)

    def one(s, carry):
        y = x_ref[pl.ds(s, lines, stride=species), :]
        y = jnp.take_along_axis(y, index, axis=1, mode="promise_in_bounds")
        top, rest = halves(y)
        mtop, mrest = halves(m_ref[s])
        dot = functools.partial(jnp.dot, preferred_element_type=jnp.float32)
        out = dot(top, mtop) + dot(rest, mtop) + dot(top, mrest)
        o_ref[pl.ds(s, lines, stride=species), :] = out
        return carry

    lax.fori_loop(0, species, one, 0, unroll=4)


def chem_kernel(chunk, y_ref, mid_ref, a_ref, turns_ref, counts_ref, owner_ref, rank_ref, from_ref, o_ref, send_ref, other_ref):
    lines, species, points = y_ref.shape
    lane = lax.broadcasted_iota(jnp.int32, (species, points), 1)
    send_ref[...] = jnp.zeros_like(send_ref)
    mid = mid_ref[...]

    def lift(l, carry):
        add = jnp.take_along_axis(mid, jnp.full((species, points), l, jnp.int32), axis=1, mode="promise_in_bounds")
        o_ref[l] = y_ref[l] + relax_rate * add
        return carry

    lax.fori_loop(0, lines, lift, 0, unroll=8)
    matrix = a_ref[...]

    def substep(sub, in_ref, out_ref):
        def part(c, inner):
            base = c * chunk
            for q in range(0, chunk, 4):
                columns = []
                state = []
                for h in (0, 2):
                    y = in_ref[pl.ds(base + q + h, 2)].reshape(2 * species, points)
                    state.append(y)
                    top, rest = halves(jnp.tanh(y))
                    columns.append(jnp.concatenate([top, top, rest], axis=0))
                right = jnp.concatenate(columns, axis=1)
                change = jnp.dot(matrix, right, preferred_element_type=jnp.float32)
                for h in (0, 1):
                    for k in (0, 1):
                        l = base + q + 2 * h + k
                        factor = jnp.where(counts_ref[l] > sub, jnp.float32(1.0), jnp.float32(0.0))
                        rows = slice(k * species, (k + 1) * species)
                        out_ref[l] = state[h][rows] + factor * change[rows, h * points : (h + 1) * points]
            return inner

        lax.fori_loop(0, lines // chunk, part, 0)

    def two(pair, carry):
        substep(2 * pair, o_ref, other_ref)
        substep(2 * pair + 1, other_ref, o_ref)
        return carry

    lax.fori_loop(0, (turns_ref[0] + 1) // 2, two, 0)

    def pack(l, carry):
        slot = rank_ref[l]
        owner = owner_ref[l]
        move = (SEG * (slot - from_ref[l])) & (points - 1)
        value = pltpu.roll(o_ref[l], move, 1)
        send_ref[owner] = jnp.where(lane // SEG == slot, value, send_ref[owner])
        return carry

    lax.fori_loop(0, lines, pack, 0, unroll=8)


def swap_kernel(names, groups, pairs, *refs):
    sends, takes = refs[:pairs], refs[pairs : 2 * pairs]
    send_sem, recv_sem, own_sem = refs[2 * pairs :]
    width = lax.axis_size(names[1])
    me = lax.axis_index(names[0]) * width + lax.axis_index(names[1])

    def place(j):
        peer = lax.rem(me + j, groups)
        return peer, (peer // width, lax.rem(peer, width))

    barrier = pltpu.get_barrier_semaphore()

    def greet(j, carry):
        pl.semaphore_signal(barrier, inc=1, device_id=place(j)[1], device_id_type=pl.DeviceIdType.MESH)
        return carry

    lax.fori_loop(1, groups, greet, 0)
    own = [pltpu.make_async_copy(sends[p].at[me], takes[p].at[me], own_sem.at[p]) for p in range(pairs)]
    for copy in own:
        copy.start()
    pl.semaphore_wait(barrier, groups - 1)

    def copies(j):
        peer, device = place(j)
        return [
            pltpu.make_async_remote_copy(
                src_ref=sends[p].at[peer],
                dst_ref=takes[p].at[me],
                send_sem=send_sem.at[p, j],
                recv_sem=recv_sem.at[p, j],
                device_id=device,
                device_id_type=pl.DeviceIdType.MESH,
            )
            for p in range(pairs)
        ]

    def begin(j, carry):
        for copy in copies(j):
            copy.start()
        return carry

    def finish(j, carry):
        for copy in copies(j):
            copy.wait()
        return carry

    lax.fori_loop(1, groups, begin, 0)
    for copy in own:
        copy.wait()
    lax.fori_loop(1, groups, finish, 0)


def swap(arrays, number):
    names = ("grid", "line")
    groups = arrays[0].shape[0]
    pairs = len(arrays)
    return pl.pallas_call(
        functools.partial(swap_kernel, names, groups, pairs),
        out_shape=[jax.ShapeDtypeStruct(a.shape, a.dtype) for a in arrays],
        in_specs=[VMEM] * pairs,
        out_specs=[VMEM] * pairs,
        scratch_shapes=[
            pltpu.SemaphoreType.DMA((pairs, groups)),
            pltpu.SemaphoreType.DMA((pairs, groups)),
            pltpu.SemaphoreType.DMA((pairs,)),
        ],
        compiler_params=pltpu.CompilerParams(collective_id=number, has_side_effects=True),
        name="swap%d" % number,
    )(*arrays)


def land_kernel(step, slots, y_ref, recv_ref, aim_ref, mid_ref, o_ref, les_ref):
    lines, species, points = y_ref.shape
    groups = recv_ref.shape[0]
    segments = points // SEG
    lane = lax.broadcasted_iota(jnp.int32, (species, points), 1)
    o_ref[...] = y_ref[...]

    def land(r, carry):
        got = recv_ref[r]
        for k in range(slots):
            code = aim_ref[r, 0, step * slots + k]
            safe = jnp.maximum(code, 0)
            line = safe // segments
            seg = safe - line * segments
            value = pltpu.roll(got, (SEG * (seg - k)) & (points - 1), 1)
            hit = lane // SEG == jnp.where(code >= 0, seg, -1)
            o_ref[line] = o_ref[line] + jnp.where(hit, splice_weight * (value - y_ref[line]), 0.0)
        return carry

    lax.fori_loop(0, groups, land, 0)

    def filtered(l, total):
        return jnp.where(lane == l, jnp.sum(o_ref[l], axis=1, keepdims=True), total)

    total = lax.fori_loop(0, lines, filtered, jnp.zeros((species, points), jnp.float32), unroll=8)
    les_ref[...] = 0.5 * mid_ref[...] + (0.5 / points) * total


def body(
    les,
    lines,
    triplet_start,
    splice_owner,
    splice_line,
    splice_from,
    splice_to,
    chem_counts,
    diffusivity,
    rates,
    frozen_inverse,
):
    groups = lax.axis_size("grid") * lax.axis_size("line")
    _, _, count, species, points = lines.shape
    segments = points // SEG
    slots = min(segments, max(2, 2 * count // groups))
    f32 = jnp.float32
    params = pltpu.CompilerParams(vmem_limit_bytes=40 * 1024 * 1024)

    mixing = diffusion_inverse(diffusivity, points) - relax_rate / points
    joint = jnp.dot(frozen_inverse, rates, precision=lax.Precision.HIGHEST)
    twice = jnp.kron(jnp.eye(2, dtype=f32), joint)
    top = lax.reduce_precision(twice, 8, 7)
    rest = lax.reduce_precision(twice - top, 8, 7)
    matrix = jnp.concatenate([top, rest, top], axis=1).astype(jnp.bfloat16)

    starts = triplet_start.reshape(STEPS, count, 1)
    owner = splice_owner.reshape(STEPS, count)
    line_to = splice_line.reshape(STEPS, count)
    seg_from = splice_from.reshape(STEPS, count)
    seg_to = splice_to.reshape(STEPS, count)
    counts = chem_counts.reshape(count)
    turns = jnp.max(counts).reshape(1)
    order = jnp.arange(count)
    earlier = (owner[:, :, None] == owner[:, None, :]) & (order[None, :, None] > order[None, None, :])
    rank = jnp.sum(earlier.astype(jnp.int32), axis=2)
    position = owner * slots + rank
    code = line_to * segments + seg_to
    hit = jnp.arange(groups * slots)[None, :, None] == position[:, None, :]
    aims = jnp.max(jnp.where(hit, code[:, None, :], -1), axis=2)
    aims = aims.reshape(STEPS, groups, slots).transpose(1, 0, 2).reshape(groups, 1, STEPS * slots)
    aims = jnp.pad(aims, ((0, 0), (0, 0), (0, points - STEPS * slots)))

    diffuse = pl.pallas_call(
        functools.partial(diffuse_kernel, species),
        out_shape=jax.ShapeDtypeStruct((count * species, points), f32),
        in_specs=[VMEM] * 3,
        out_specs=VMEM,
        compiler_params=params,
        cost_estimate=pl.CostEstimate(flops=6 * species * count * points * points, bytes_accessed=5 << 20, transcendentals=0),
        name="diffuse",
    )
    block = jax.ShapeDtypeStruct((count, species, points), f32)
    chem = pl.pallas_call(
        functools.partial(chem_kernel, 64),
        out_shape=(block, jax.ShapeDtypeStruct((groups, species, points), f32)),
        in_specs=[VMEM] * 3 + [SMEM] * 5,
        out_specs=(VMEM, VMEM),
        scratch_shapes=[pltpu.VMEM((count, species, points), f32)],
        compiler_params=params,
        name="chem",
    )
    def land(step, *given):
        return pl.pallas_call(
            functools.partial(land_kernel, step, slots),
            out_shape=(block, jax.ShapeDtypeStruct((species, count), f32)),
            in_specs=[VMEM, VMEM, SMEM, VMEM],
            out_specs=(VMEM, VMEM),
            compiler_params=params,
            name="land",
        )(*given)

    field = les
    state = lines.reshape(count, species, points)
    for step in range(STEPS):
        beside = neighbours(field, STEPS + step)
        mid = (field + les_rate * (beside - 4.0 * field)).reshape(species, count)
        spread = diffuse(state.reshape(count * species, points), starts[step], mixing)
        state, sending = chem(
            spread.reshape(count, species, points), mid, matrix, turns, counts, owner[step], rank[step], seg_from[step]
        )
        if step == 0:
            received, aims = swap([sending, aims], 0)
        else:
            (received,) = swap([sending], step)
        state, field = land(step, state, received, aims, mid)
        field = field.reshape(les.shape)
    return (field, state.reshape(lines.shape))


def solution(mesh):
    in_specs = (
        P(None, "grid", "line"),
        P("grid", "line", None, None, None),
        P(None, "grid", "line", None),
        P(None, "grid", "line", None, None),
        P(None, "grid", "line", None),
        P(None, "grid", "line", None),
        P(None, "grid", "line", None),
        P("grid", "line", None),
        P(),
        P(),
        P(),
    )
    out_specs = (P(None, "grid", "line"), P("grid", "line", None, None, None))
    return jax.shard_map(body, mesh=mesh, in_specs=in_specs, out_specs=out_specs, check_vma=False)
```
